32 devices in a mesh: angle: 2 (over y), ty: 8 (over z, core), tx: 2 (over x).
Axes of the slice: x: 2, y: 2, z: 4, core: 2. Of those that a mesh axis runs over, the one named last changes fastest.
Arguments:
- object_slices: float32 [2, 2, 2048, 2048], P('angle', None, 'ty', 'tx'), may hold values from -5 to 5
- probe_field: float32 [2, 256, 256], replicated, may hold values from -6 to 6
- positions: int32 [2, 8, 2, 4, 2], P('angle', 'ty', 'tx'), may hold values from 0 to 1792, as said below
- live_slots: int32 [2, 8, 2], P('angle', 'ty', 'tx'), may hold values from 1 to 4, as said below
- photon_counts: int32 [2, 8, 2, 4, 256, 256], P('angle', 'ty', 'tx'), may hold values from 1 to 1600
Outputs:
- new_object: float32 [2, 2, 2048, 2048], P('angle', None, 'ty', 'tx')
- new_probe: float32 [2, 256, 256], P(None, 'ty')
The draws below stay inside these ranges and needn't reach their ends.
Inputs may be any that keep to these rules, and one draw needn't show every extreme that they name: `positions`: A slot's patch lies inside the object and its centre (top-left plus 128) lies in the rows and columns of the tile that holds the slot: rows r * 256 to (r + 1) * 256 - 1, columns c * 1024 to (c + 1) * 1024 - 1. `live_slots`: some tile of every draw uses all 4 slots.
All inputs are finite; a program needn't handle non-finite values.
Results may differ from the reference program's by a relative error of at most 0.0003.
Values sent between devices are 32-bit elements; how exact they have to be, the bound alone decides.
A program may use at most 128 MiB of HBM per device.

```python
import jax
import jax.numpy as jnp
from jax import lax

P_SIZE = 256
TR = 256
TC = 1024
SLOTS = 4
ANGLES = 2
NR = 2048
NC = 2048
N_TY = 8
N_TX = 2


def draw_positions(key, part):
    shape = (ANGLES, N_TY, N_TX, SLOTS)
    first_key, second_key = jax.random.split(jax.random.fold_in(key, 11))
    row_draw = jax.random.randint(first_key, shape, 0, TR)
    col_draw = jax.random.randint(second_key, shape, 0, TC)
    tile_row = lax.broadcasted_iota(jnp.int32, shape, 1)
    tile_col = lax.broadcasted_iota(jnp.int32, shape, 2)
    row_start = jnp.clip(tile_row * TR - P_SIZE // 2 + row_draw, 0, NR - P_SIZE)
    col_start = jnp.clip(tile_col * TC - P_SIZE // 2 + col_draw, 0, NC - P_SIZE)
    return jnp.stack([row_start, col_start], axis=-1).astype(jnp.int32)


def draw_live_slots(key, part):
    shape = (ANGLES, N_TY, N_TX)
    first_key, second_key, third_key = jax.random.split(jax.random.fold_in(key, 23), 3)
    sparse = jax.random.randint(first_key, shape, 1, max(SLOTS // 4, 1) + 1)
    dense = jax.random.randint(second_key, shape, 0, 8) == 0
    values = jnp.where(dense, SLOTS, sparse).reshape(-1)
    chosen = jax.random.randint(third_key, (), 0, ANGLES * N_TY * N_TX)
    values = jnp.where(jnp.arange(ANGLES * N_TY * N_TX) == chosen, SLOTS, values)
    return values.reshape(shape).astype(jnp.int32)


def set_ends(result, own_key, smallest, high):
    longest = result.shape.index(max(result.shape))
    spots = []
    for shift in (0, 1):
        where = [jax.random.randint(jax.random.fold_in(own_key, axis), (), 0, length) for axis, length in enumerate(result.shape)]
        where[longest] = (where[longest] + shift) % result.shape[longest]
        spots.append(tuple(where))
    return result.at[spots[0]].set(smallest).at[spots[1]].set(high)


def block_scale(stream_key, shape, cuts, smallest, largest):
    level, own = 1.0, jax.random.fold_in(stream_key, 6)
    for axis_at, parts in cuts:
        draws = jnp.exp(jax.random.uniform(jax.random.fold_in(own, axis_at), (parts,), jnp.float32, smallest / len(cuts), largest / len(cuts)))
        level = level * jnp.repeat(draws, shape[axis_at] // parts).reshape([-1 if axis == axis_at else 1 for axis in range(len(shape))])
    return level


def noise(stream_key, extent, width, limit, pieces=(), kind=jnp.bfloat16):
    gain = block_scale(stream_key, extent, pieces, -0.22, 0.18) if pieces else 1.0
    values = jax.random.normal(stream_key, extent, jnp.float32) * width * gain
    return jnp.minimum(jnp.maximum(values, -limit), limit).astype(kind)


def setup_inputs(seed: int = 0) -> dict:
    key_of = jax.random.split(jax.random.key(seed), 6)
    object_slices = noise(key_of[0], (ANGLES, 2, NR, NC), 0.7, 5.0, ((0, 2), (2, 8), (3, 2)), jnp.float32)
    probe_field = noise(key_of[1], (2, P_SIZE, P_SIZE), 1.0, 6.0, (), jnp.float32)
    positions = draw_positions(jax.random.fold_in(key_of[5], 71), 0)
    live_slots = draw_live_slots(jax.random.fold_in(key_of[5], 71), 0)
    photon_counts = set_ends(jax.random.randint(key_of[4], (ANGLES, N_TY, N_TX, SLOTS, P_SIZE, P_SIZE), 1, 1601), jax.random.fold_in(key_of[4], 1), 1, 1600).astype(jnp.int32)
    return {"object_slices": object_slices, "probe_field": probe_field, "positions": positions, "live_slots": live_slots, "photon_counts": photon_counts}


def reference(object_slices, probe_field, positions, live_slots, photon_counts):
    ftype = object_slices.dtype
    probe_wave = lax.complex(probe_field[0], probe_field[1])
    probe_power = probe_field[0] * probe_field[0] + probe_field[1] * probe_field[1]
    slot_index = jnp.arange(SLOTS, dtype=jnp.int32)
    probe_num = jnp.zeros((P_SIZE, P_SIZE), probe_wave.dtype)
    probe_den = jnp.zeros((P_SIZE, P_SIZE), ftype)
    numerators = []
    denominators = []
    fields = []
    for angle_index in range(ANGLES):
        field = lax.complex(object_slices[angle_index, 0], object_slices[angle_index, 1])
        spots = positions[angle_index].reshape(-1, 2).astype(jnp.int32)
        weights = (slot_index[None, None, :] < live_slots[angle_index][:, :, None]).astype(ftype).reshape(-1)
        measured = photon_counts[angle_index].reshape(-1, P_SIZE, P_SIZE)

        def deposit(carry, item):
            obj_num, obj_den, pr_num, pr_den = carry
            spot, weight, count = item
            row_at = spot[0].astype(jnp.int32)
            col_at = spot[1].astype(jnp.int32)
            patch = lax.dynamic_slice(field, (row_at, col_at), (P_SIZE, P_SIZE))
            wave = probe_wave * patch
            far = jnp.fft.fft2(wave, norm='ortho')
            amplitude = 0.05 * jnp.sqrt(count.astype(ftype))
            factor = amplitude * lax.rsqrt(jnp.maximum(far.real * far.real + far.imag * far.imag, 0.0625))
            gap = (jnp.fft.ifft2(far * factor, norm='ortho') - wave) * weight
            current = lax.dynamic_slice(obj_num, (row_at, col_at), (P_SIZE, P_SIZE))
            obj_num = lax.dynamic_update_slice(obj_num, current + jnp.conj(probe_wave) * gap, (row_at, col_at))
            current_den = lax.dynamic_slice(obj_den, (row_at, col_at), (P_SIZE, P_SIZE))
            obj_den = lax.dynamic_update_slice(obj_den, current_den + weight * probe_power, (row_at, col_at))
            pr_num = pr_num + jnp.conj(patch) * gap
            pr_den = pr_den + weight * (patch.real * patch.real + patch.imag * patch.imag)
            return ((obj_num, obj_den, pr_num, pr_den), None)
        start = (jnp.zeros(field.shape, field.dtype), jnp.zeros(field.shape, ftype), probe_num, probe_den)
        (obj_num, obj_den, probe_num, probe_den), _ = lax.scan(deposit, start, (spots, weights, measured))
        numerators.append(obj_num)
        denominators.append(obj_den)
        fields.append(field)
    peak_obj = jnp.max(jnp.stack([jnp.max(den) for den in denominators]))
    peak_probe = jnp.max(probe_den)
    updated = []
    for angle_index in range(ANGLES):
        value = fields[angle_index] + numerators[angle_index] / (denominators[angle_index] + 0.1 * peak_obj)
        updated.append(jnp.stack([value.real, value.imag]))
    new_object = jnp.stack(updated)
    probe_new = probe_wave + probe_num / (probe_den + 0.1 * peak_probe)
    new_probe = jnp.stack([probe_new.real, probe_new.imag])
    return (new_object, new_probe)
```

```python
import functools
import math

import jax
import jax.numpy as jnp
import numpy as np
from jax import lax
from jax.experimental import pallas as pl
from jax.experimental.pallas import tpu as pltpu
from jax.sharding import PartitionSpec as P

MESH = pl.DeviceIdType.MESH
VMEM_LIMIT = 56 * 1024 * 1024
AROUND = tuple((dy, dx) for dy in (-1, 0, 1) for dx in (-1, 0, 1))
BESIDE = tuple(d for d in AROUND if d != (0, 0))


def slot_of(dy, dx):
    return (dy + 1) * 3 + dx + 1


def present(dy, dx, shape):
    row = lax.axis_index("ty") + dy
    col = lax.axis_index("tx") + dx
    return (row >= 0) & (row < shape["ty"]) & (col >= 0) & (col < shape["tx"])


def beside_counts(shape):
    found = []
    for axis in ("ty", "tx"):
        at = lax.axis_index(axis)
        found.append(jnp.where(at > 0, 1, 0) + jnp.where(at < shape[axis] - 1, 1, 0))
    return found


def neighbour(dy, dx):
    return {"ty": lax.axis_index("ty") + dy, "tx": lax.axis_index("tx") + dx}


def edge_part(step, size, half):
    return {-1: slice(0, half), 0: slice(0, size), 1: slice(size - half, size)}[step]


def wide_part(step, size, half):
    return {
        -1: slice(0, half),
        0: slice(half, half + size),
        1: slice(half + size, size + 2 * half),
    }[step]


def at2(ref, rows, cols):
    return ref.at[:, pl.ds(rows.start, rows.stop - rows.start), pl.ds(cols.start, cols.stop - cols.start)]


def halo_kernel(shape, half, tile, meta, wide, metas, send, recv, msend, mrecv, local):
    rows, cols = tile.shape[1], tile.shape[2]
    barrier = pltpu.get_barrier_semaphore()
    for dy, dx in BESIDE:
        @pl.when(present(dy, dx, shape))
        def _():
            pl.semaphore_signal(barrier, inc=1, device_id=neighbour(dy, dx), device_id_type=MESH)
    centre = at2(wide, wide_part(0, rows, half), wide_part(0, cols, half))
    own = pltpu.make_async_copy(tile, centre, local.at[0])
    own.start()
    own_meta = pltpu.make_async_copy(meta, metas.at[4], local.at[1])
    own_meta.start()
    n_row, n_col = beside_counts(shape)
    pl.semaphore_wait(barrier, n_row + n_col + n_row * n_col)

    def copies(dy, dx, k):
        src = at2(tile, edge_part(dy, rows, half), edge_part(dx, cols, half))
        dst = at2(wide, wide_part(-dy, rows, half), wide_part(-dx, cols, half))
        data = pltpu.make_async_remote_copy(
            src_ref=src, dst_ref=dst, send_sem=send.at[k], recv_sem=recv.at[k],
            device_id=neighbour(dy, dx), device_id_type=MESH)
        note = pltpu.make_async_remote_copy(
            src_ref=meta, dst_ref=metas.at[slot_of(-dy, -dx)], send_sem=msend.at[k],
            recv_sem=mrecv.at[k], device_id=neighbour(dy, dx), device_id_type=MESH)
        return data, note

    order = sorted(BESIDE, key=lambda d: abs(d[1]))
    for dy, dx in order:
        @pl.when(present(dy, dx, shape))
        def _():
            data, note = copies(dy, dx, slot_of(dy, dx))
            data.start()
            note.start()
    for dy, dx in order:
        @pl.when(present(dy, dx, shape))
        def _():
            data, note = copies(dy, dx, slot_of(dy, dx))
            data.wait_send()
            note.wait_send()
            data, note = copies(-dy, -dx, slot_of(-dy, -dx))
            data.wait_recv()
            note.wait_recv()
    own.wait()
    own_meta.wait()


def split(value):
    high = value.astype(jnp.bfloat16)
    low = (value - high.astype(jnp.float32)).astype(jnp.bfloat16)
    return high, low


def mm(a, b):
    return lax.dot_general(a, b, (((1,), (0,)), ((), ())), preferred_element_type=jnp.float32)


def compute_kernel(shape, tile_rows, tile_cols, metas, wide_in, probe, counts, tables,
                   tot_out, den, den_max, sums, acc, denbuf, u_hi, u_lo, v_hi, v_lo, wide, tot,
                   load_sem, save_sem):
    size = probe.shape[1]
    half = size // 2
    blocks = wide.shape[1]

    def strip(ref, j):
        return ref.at[:, :, pl.ds(j * 128, 128)]

    def load(j):
        return pltpu.make_async_copy(strip(wide_in, j), wide.at[:, j], load_sem.at[j])

    def save(j):
        return pltpu.make_async_copy(tot.at[:, j], strip(tot_out, j), save_sem.at[j])

    for j in range(blocks):
        load(j).start()
    slots = counts.shape[0]
    ty, tx = lax.axis_index("ty"), lax.axis_index("tx")
    for n, (u, v) in enumerate(((u_hi, v_hi), (u_lo, v_lo))):
        c, s = tables[2 * n], tables[2 * n + 1]
        u[0:size, 0:size] = c
        u[0:size, size:] = s
        u[size:, 0:size] = -s
        u[size:, size:] = c
        v[0:size, 0:size] = c
        v[0:size, size:] = -s
        v[size:, 0:size] = s
        v[size:, size:] = c
    tot[...] = jnp.zeros_like(tot)
    acc[...] = jnp.zeros_like(acc)
    edge = size // 128
    inner = slice(edge, edge + tile_cols // 128)
    denbuf[inner, size:size + tile_rows, :] = jnp.zeros((tile_cols // 128, tile_rows, 128), jnp.float32)
    pad = jnp.zeros((size, 128), jnp.float32)
    wider = size + 128

    def spread(piece, shift):
        return pltpu.roll(jnp.concatenate([piece, pad], axis=1), shift, axis=1)

    def from_left(m_hi, m_lo, re, im):
        hi, lo = split(jnp.concatenate([re, im], axis=0))
        out = mm(m_hi[...], hi) + (mm(m_hi[...], lo) + mm(m_lo[...], hi))
        return out[:size], out[size:]

    def from_right(m_hi, m_lo, re, im):
        hi, lo = split(jnp.concatenate([re, im], axis=1))
        out = mm(hi, m_hi[...]) + (mm(lo, m_hi[...]) + mm(hi, m_lo[...]))
        return out[:, :size], out[:, size:]

    def one_den(n, carry):
        k, s = n // slots, n % slots
        row = metas[k, 0, s] - ty * tile_rows
        col = metas[k, 0, slots + s] - tx * tile_cols
        there_r, there_c = ty + k // 3 - 1, tx + k % 3 - 1
        there = (there_r >= 0) & (there_r < shape["ty"]) & (there_c >= 0) & (there_c < shape["tx"])
        meets = (row > -size) & (row < tile_rows) & (col > -size) & (col < tile_cols)

        @pl.when(there & meets & (s < metas[k, 0, 2 * slots]))
        def _():
            q = probe[0] * probe[0] + probe[1] * probe[1]
            at = col + size
            value = spread(q, at % 128)
            for i in range(wider // 128):
                where = (at // 128 + i, pl.ds(row + size, size), slice(None))
                denbuf[where] += value[:, i * 128:(i + 1) * 128]
        return carry

    lax.fori_loop(0, 9 * slots, one_den, 0)
    own = denbuf[inner, size:size + tile_rows, :]
    for j in range(tile_cols // 128):
        den[:, j * 128:(j + 1) * 128] = own[j]
    most = jnp.max(own, axis=0)
    den_max[...] = jnp.broadcast_to(jnp.max(jnp.max(most, axis=0, keepdims=True), axis=1, keepdims=True), den_max.shape)
    for j in range(blocks):
        load(j).wait()

    def one_slot(s, carry):
        row = metas[4, 0, s] - ty * tile_rows + half
        at = metas[4, 0, slots + s] - tx * tile_cols + half
        first = at // 128
        shift = at % 128
        back_shift = (wider - shift) % wider

        def patch(ch):
            found = [wide[ch, first + i, pl.ds(row, size), :] for i in range(wider // 128)]
            return pltpu.roll(jnp.concatenate(found, axis=1), back_shift, axis=1)[:, :size]

        def deposit(ch, piece):
            value = spread(piece, shift)
            for i in range(wider // 128):
                tot[ch, first + i, pl.ds(row, size), :] += value[:, i * 128:(i + 1) * 128]

        x_re, x_im = patch(0), patch(1)
        q_re, q_im = probe[0], probe[1]
        p_re = q_re * x_re - q_im * x_im
        p_im = q_re * x_im + q_im * x_re
        f_re, f_im = from_right(v_hi, v_lo, *from_left(u_hi, u_lo, p_re, p_im))
        amplitude = 0.05 * jnp.sqrt(counts[s].astype(jnp.float32))
        factor = amplitude * lax.rsqrt(jnp.maximum(f_re * f_re + f_im * f_im, 0.0625))
        b_re, b_im = from_right(u_hi, u_lo, *from_left(v_hi, v_lo, f_re * factor, f_im * factor))
        d_re, d_im = b_re - p_re, b_im - p_im
        deposit(0, q_re * d_re + q_im * d_im)
        deposit(1, q_re * d_im - q_im * d_re)
        acc[0] += x_re * d_re + x_im * d_im
        acc[1] += x_re * d_im - x_im * d_re
        acc[2] += x_re * x_re + x_im * x_im
        return carry

    lax.fori_loop(0, metas[4, 0, 2 * slots], one_slot, 0)
    for j in range(blocks):
        save(j).start()
    each = size // shape["ty"]
    for t in range(shape["ty"]):
        for ch in range(3):
            sums[t % 2, t // 2, ch * each:(ch + 1) * each, :] = acc[ch, t * each:(t + 1) * each, :]
    for j in range(blocks):
        save(j).wait()


def fold_kernel(shape, half, tile, tot, den, den_max, sums, probe_rows, out, out_probe,
                centre, rim_v, rim_h, rim_c, r1, s1, r2, s2, r3, s3, g4, pk_a, pk_b, pk_c,
                fsend, frecv, send1, recv1, send2, recv2, send3, recv3, send4, recv4,
                ksend, krecv, lsend, lrecv, msend, mrecv, local):
    rows, cols = tile.shape[1], tile.shape[2]
    n_ty, n_tx, n_an = shape["ty"], shape["tx"], shape["angle"]
    ty, tx, an = lax.axis_index("ty"), lax.axis_index("tx"), lax.axis_index("angle")
    core, z = ty % 2, ty // 2
    n_z = n_ty // 2
    group = n_an * n_tx
    gid = an * n_tx + tx
    part = sums.shape[3] // n_an
    diagonals = [d for d in BESIDE if d[0] and d[1]]
    barrier = pltpu.get_barrier_semaphore()

    def signal(where):
        pl.semaphore_signal(barrier, inc=1, device_id=where, device_id_type=MESH)

    def member(d):
        g = (gid + d) % group
        return g, {"angle": g // n_tx, "tx": g % n_tx}

    for d in range(1, n_ty):
        signal({"ty": (ty + d) % n_ty})
    for d in range(1, group):
        signal(member(d)[1])
    for dy, dx in diagonals:
        @pl.when(present(dy, dx, shape))
        def _():
            signal(neighbour(dy, dx))
    load = pltpu.make_async_copy(
        at2(tot, wide_part(0, rows, half), wide_part(0, cols, half)), centre, local.at[0])
    load.start()
    n_row, n_col = beside_counts(shape)
    pl.semaphore_wait(barrier, n_ty - 1 + group - 1 + n_row * n_col)

    def rdma(src, dst, s_sem, r_sem, where):
        return pltpu.make_async_remote_copy(
            src_ref=src, dst_ref=dst, send_sem=s_sem, recv_sem=r_sem,
            device_id=where, device_id_type=MESH)

    def landing(dy, dx):
        if dx == 0:
            return rim_v.at[(dy + 1) // 2]
        if dy == 0:
            return rim_h.at[(dx + 1) // 2]
        return rim_c.at[(dy + 1) + (dx + 1) // 2]

    def fold(dy, dx):
        k = slot_of(dy, dx)
        src = at2(tot, wide_part(dy, rows, half), wide_part(dx, cols, half))
        return rdma(src, landing(dy, dx), fsend.at[k], frecv.at[k], neighbour(dy, dx))

    pair = {"ty": ty + 1 - 2 * core}
    c1 = rdma(sums.at[1 - core], r1, send1.at[0], recv1.at[0], pair)
    c1.start()
    for d in range(1, group):
        g, where = member(d)
        rdma(den_max, pk_a.at[gid], ksend.at[d], krecv.at[gid], where).start()
    for dy, dx in sorted(BESIDE, key=lambda d: abs(d[1])):
        @pl.when(present(dy, dx, shape))
        def _():
            fold(dy, dx).start()

    pk_a[pl.ds(gid, 1)] = den_max[...][None]
    c1.wait()
    s1[...] = sums[core] + r1[...]

    def lanes(ref, a):
        return ref.at[:, :, pl.ds(pl.multiple_of(a * part, part), part)]

    def stage2(d):
        a = (an + d) % n_an
        return rdma(lanes(s1, a), r2.at[an], send2.at[d], recv2.at[an], {"angle": a})

    for d in range(1, n_an):
        stage2(d).start()
    for d in range(1, group):
        g, where = member(d)
        rdma(den_max, pk_a.at[g], ksend.at[d], krecv.at[g], where).wait()
    peak = pk_a[0]
    for g in range(1, group):
        peak = jnp.maximum(peak, pk_a[g])
    pk_b[pl.ds(ty, 1)] = peak[None]
    for d in range(1, n_ty):
        rdma(pk_b.at[ty], pk_b.at[ty], lsend.at[d], lrecv.at[ty], {"ty": (ty + d) % n_ty}).start()
    for d in range(1, n_an):
        a = (an + d) % n_an
        rdma(lanes(s1, a), r2.at[a], send2.at[d], recv2.at[a], {"angle": a}).wait()
    mine = s1[:, :, pl.ds(pl.multiple_of(an * part, part), part)]
    for d in range(1, n_an):
        mine = mine + r2[(an + d) % n_an]
    s2[...] = mine

    for d in range(1, n_z):
        o = (z + d) % n_z
        rdma(s2.at[o], r3.at[z], send3.at[d], recv3.at[z], {"ty": o * 2 + core}).start()
    for d in range(1, n_z):
        o = (z + d) % n_z
        rdma(s2.at[o], r3.at[o], send3.at[d], recv3.at[o], {"ty": o * 2 + core}).wait()
    total = s2[z]
    for d in range(1, n_z):
        total = total + r3[(z + d) % n_z]
    s3[...] = total
    g4[pl.ds(gid, 1)] = total[None]

    for d in range(1, group):
        g, where = member(d)
        rdma(s3, g4.at[gid], send4.at[d], recv4.at[gid], where).start()
    for d in range(1, group):
        g, where = member(d)
        rdma(s3, g4.at[g], send4.at[d], recv4.at[g], where).wait()
    pieces = []
    for a in range(n_an):
        piece = g4[a * n_tx]
        for t in range(1, n_tx):
            piece = piece + g4[a * n_tx + t]
        pieces.append(piece)
    full = jnp.concatenate(pieces, axis=1)
    each = full.shape[0] // 3
    p_re, p_im, p_den = full[:each], full[each:2 * each], full[2 * each:]

    def top(value):
        return jnp.max(jnp.max(value, axis=0, keepdims=True), axis=1, keepdims=True)

    pk_c[pl.ds(ty, 1)] = jnp.broadcast_to(top(p_den), den_max.shape)[None]
    for d in range(1, n_ty):
        rdma(pk_c.at[ty], pk_c.at[ty], msend.at[d], mrecv.at[ty], {"ty": (ty + d) % n_ty}).start()

    load.wait()
    for dy, dx in sorted(BESIDE, key=lambda d: -abs(d[1])):
        @pl.when(present(dy, dx, shape))
        def _():
            fold(dy, dx).wait_send()
            fold(-dy, -dx).wait_recv()
            r, c = edge_part(dy, rows, half), edge_part(dx, cols, half)
            centre[:, r, c] += landing(-dy, -dx)[...]
    for d in range(1, n_ty):
        o = (ty + d) % n_ty
        rdma(pk_b.at[ty], pk_b.at[o], lsend.at[d], lrecv.at[o], {"ty": o}).wait()
    peak = pk_b[0]
    for t in range(1, n_ty):
        peak = jnp.maximum(peak, pk_b[t])
    scale = 1.0 / (den[...] + 0.1 * peak[0:1, 0:1])
    out[0] = tile[0] + centre[0] * scale
    out[1] = tile[1] + centre[1] * scale

    for d in range(1, n_ty):
        o = (ty + d) % n_ty
        rdma(pk_c.at[ty], pk_c.at[o], msend.at[d], mrecv.at[o], {"ty": o}).wait()
    peak = pk_c[0]
    for t in range(1, n_ty):
        peak = jnp.maximum(peak, pk_c[t])
    scale = 1.0 / (p_den + 0.1 * peak[0:1, 0:1])
    out_probe[0] = probe_rows[0] + p_re * scale
    out_probe[1] = probe_rows[1] + p_im * scale


def table_values(length):
    ids = np.arange(length)
    phase = 2.0 * math.pi / length * (np.outer(ids, ids) % length)
    cos, sin = np.cos(phase) / math.sqrt(length), np.sin(phase) / math.sqrt(length)
    parts = []
    for value in (cos, sin):
        high = value.astype(jnp.bfloat16)
        low = (value - high.astype(np.float64)).astype(jnp.bfloat16)
        parts.append((high, low))
    return np.stack([parts[0][0], parts[1][0], parts[0][1], parts[1][1]])


def body(shape, object_slices, probe_field, positions, live_slots, photon_counts):
    f32 = jnp.float32
    dma = pltpu.SemaphoreType.DMA
    size = probe_field.shape[1]
    half = size // 2
    tile = object_slices[0]
    _, rows, cols = tile.shape
    spots = positions[0, 0, 0]
    slots = spots.shape[0]
    vmem = pl.BlockSpec(memory_space=pltpu.VMEM)
    smem = pl.BlockSpec(memory_space=pltpu.SMEM)
    anywhere = pl.BlockSpec(memory_space=pl.ANY)
    line = jnp.concatenate([spots[:, 0], spots[:, 1], live_slots[0, 0]])
    meta = jnp.broadcast_to(jnp.pad(line, (0, 128 - line.shape[0]))[None], (8, 128))
    wide, metas = pl.pallas_call(
        functools.partial(halo_kernel, shape, half),
        out_shape=(
            jax.ShapeDtypeStruct((2, rows + size, cols + size), f32),
            jax.ShapeDtypeStruct((9, 8, 128), jnp.int32),
        ),
        in_specs=[vmem, vmem],
        out_specs=(anywhere, anywhere),
        scratch_shapes=[dma((9,)), dma((9,)), dma((9,)), dma((9,)), dma((2,))],
        compiler_params=pltpu.CompilerParams(
            collective_id=0, has_side_effects=True, vmem_limit_bytes=VMEM_LIMIT),
    )(tile, meta)

    n_ty, n_tx, n_an = shape["ty"], shape["tx"], shape["angle"]
    n_z, each, group = n_ty // 2, size // n_ty, n_an * n_tx
    part = size // n_an
    tot, den, den_max, sums = pl.pallas_call(
        functools.partial(compute_kernel, shape, rows, cols),
        out_shape=(
            jax.ShapeDtypeStruct((2, rows + size, cols + size), f32),
            jax.ShapeDtypeStruct((rows, cols), f32),
            jax.ShapeDtypeStruct((8, 128), f32),
            jax.ShapeDtypeStruct((2, n_z, 3 * each, size), f32),
        ),
        in_specs=[smem, anywhere, vmem, vmem, vmem],
        out_specs=(anywhere, vmem, vmem, vmem),
        scratch_shapes=[
            pltpu.VMEM((3, size, size), f32),
            pltpu.VMEM(((cols + 2 * size) // 128, rows + 2 * size, 128), f32),
        ] + [pltpu.VMEM((2 * size, 2 * size), jnp.bfloat16)] * 4 + [
            pltpu.VMEM((2, (cols + size) // 128, rows + size, 128), f32)] * 2 + [
            dma(((cols + size) // 128,))] * 2,
        compiler_params=pltpu.CompilerParams(vmem_limit_bytes=VMEM_LIMIT),
    )(metas, wide, probe_field, photon_counts[0, 0, 0], jnp.asarray(table_values(size)))

    probe_rows = lax.dynamic_slice_in_dim(probe_field, lax.axis_index("ty") * each, each, 1)
    return pl.pallas_call(
        functools.partial(fold_kernel, shape, half),
        out_shape=(
            jax.ShapeDtypeStruct((2, rows, cols), f32),
            jax.ShapeDtypeStruct((2, each, size), f32),
        ),
        in_specs=[vmem, anywhere, vmem, vmem, vmem, vmem],
        out_specs=(vmem, vmem),
        scratch_shapes=[
            pltpu.VMEM((2, rows, cols), f32),
            pltpu.VMEM((2, 2, half, cols), f32),
            pltpu.VMEM((2, 2, rows, half), f32),
            pltpu.VMEM((4, 2, half, half), f32),
            pltpu.VMEM((n_z, 3 * each, size), f32),
            pltpu.VMEM((n_z, 3 * each, size), f32),
            pltpu.VMEM((n_an, n_z, 3 * each, part), f32),
            pltpu.VMEM((n_z, 3 * each, part), f32),
            pltpu.VMEM((n_z, 3 * each, part), f32),
            pltpu.VMEM((3 * each, part), f32),
            pltpu.VMEM((group, 3 * each, part), f32),
            pltpu.VMEM((group, 8, 128), f32),
            pltpu.VMEM((n_ty, 8, 128), f32),
            pltpu.VMEM((n_ty, 8, 128), f32),
            dma((9,)), dma((9,)), dma((1,)), dma((1,)), dma((n_an,)), dma((n_an,)),
            dma((n_z,)), dma((n_z,)), dma((group,)), dma((group,)),
            dma((group,)), dma((group,)), dma((n_ty,)), dma((n_ty,)), dma((n_ty,)), dma((n_ty,)),
            dma((1,)),
        ],
        compiler_params=pltpu.CompilerParams(
            collective_id=1, has_side_effects=True, vmem_limit_bytes=VMEM_LIMIT),
    )(tile, tot, den, den_max, sums, probe_rows)


def solution(mesh):
    shape = dict(mesh.shape)

    def step(*args):
        new_tile, new_probe = body(shape, *args)
        return new_tile[None], new_probe

    return jax.shard_map(
        step,
        mesh=mesh,
        in_specs=(
            P("angle", None, "ty", "tx"),
            P(),
            P("angle", "ty", "tx", None, None),
            P("angle", "ty", "tx"),
            P("angle", "ty", "tx", None, None, None),
        ),
        out_specs=(P("angle", None, "ty", "tx"), P(None, "ty", None)),
        check_vma=False,
    )
```

```python
import functools
import math

import jax
import jax.numpy as jnp
import numpy as np
from jax import lax
from jax.experimental import pallas as pl
from jax.experimental.pallas import tpu as pltpu
from jax.sharding import PartitionSpec as P

MESH = pl.DeviceIdType.MESH
MIB = 1024 * 1024
HALO_VMEM = 4 * MIB
VMEM_LIMIT = 32 * MIB
FOLD_VMEM = 14 * MIB
AROUND = tuple((dy, dx) for dy in (-1, 0, 1) for dx in (-1, 0, 1))
BESIDE = tuple(d for d in AROUND if d != (0, 0))


def slot_of(dy, dx):
    return (dy + 1) * 3 + dx + 1


def present(dy, dx, shape):
    row = lax.axis_index("ty") + dy
    col = lax.axis_index("tx") + dx
    return (row >= 0) & (row < shape["ty"]) & (col >= 0) & (col < shape["tx"])


def beside_counts(shape):
    found = []
    for axis in ("ty", "tx"):
        at = lax.axis_index(axis)
        found.append(jnp.where(at > 0, 1, 0) + jnp.where(at < shape[axis] - 1, 1, 0))
    return found


def neighbour(dy, dx):
    return {"ty": lax.axis_index("ty") + dy, "tx": lax.axis_index("tx") + dx}


def edge_part(step, size, half):
    return {-1: slice(0, half), 0: slice(0, size), 1: slice(size - half, size)}[step]


def wide_part(step, size, half):
    return {
        -1: slice(0, half),
        0: slice(half, half + size),
        1: slice(half + size, size + 2 * half),
    }[step]


def at2(ref, rows, cols):
    return ref.at[:, pl.ds(rows.start, rows.stop - rows.start), pl.ds(cols.start, cols.stop - cols.start)]


def halo_kernel(shape, half, tile, meta, wide, metas, send, recv, msend, mrecv, local):
    rows, cols = tile.shape[1], tile.shape[2]
    barrier = pltpu.get_barrier_semaphore()
    for dy, dx in BESIDE:
        @pl.when(present(dy, dx, shape))
        def _():
            pl.semaphore_signal(barrier, inc=1, device_id=neighbour(dy, dx), device_id_type=MESH)
    own_meta = pltpu.make_async_copy(meta, metas.at[4], local.at[1])
    own_meta.start()
    n_row, n_col = beside_counts(shape)
    pl.semaphore_wait(barrier, n_row + n_col + n_row * n_col)

    def copies(dy, dx, k):
        src = at2(tile, edge_part(dy, rows, half), edge_part(dx, cols, half))
        dst = at2(wide, wide_part(-dy, rows, half), wide_part(-dx, cols, half))
        data = pltpu.make_async_remote_copy(
            src_ref=src, dst_ref=dst, send_sem=send.at[k], recv_sem=recv.at[k],
            device_id=neighbour(dy, dx), device_id_type=MESH)
        note = pltpu.make_async_remote_copy(
            src_ref=meta, dst_ref=metas.at[slot_of(-dy, -dx)], send_sem=msend.at[k],
            recv_sem=mrecv.at[k], device_id=neighbour(dy, dx), device_id_type=MESH)
        return data, note

    order = sorted(BESIDE, key=lambda d: abs(d[1]))
    for dy, dx in order:
        @pl.when(present(dy, dx, shape))
        def _():
            data, note = copies(dy, dx, slot_of(dy, dx))
            data.start()
            note.start()
    for dy, dx in order:
        @pl.when(present(dy, dx, shape))
        def _():
            data, note = copies(dy, dx, slot_of(dy, dx))
            data.wait_send()
            note.wait_send()
            data, note = copies(-dy, -dx, slot_of(-dy, -dx))
            data.wait_recv()
            note.wait_recv()
    own_meta.wait()


def split(value):
    high = value.astype(jnp.bfloat16)
    low = (value - high.astype(jnp.float32)).astype(jnp.bfloat16)
    return high, low


def mm(a, b):
    return lax.dot_general(a, b, (((1,), (0,)), ((), ())), preferred_element_type=jnp.float32)


def compute_kernel(shape, tile_rows, tile_cols, metas, tile_in, wide_in, probe, counts, tables,
                   tot_out, den, den_max, sums, acc, denbuf, u_hi, u_lo, v_hi, v_lo, wide, tot,
                   load_sem, save_sem):
    size = probe.shape[1]
    half = size // 2
    blocks = wide.shape[1]

    def strip(ref, j):
        return ref.at[:, :, pl.ds(j * 128, 128)]

    inside = range(half // 128, blocks - half // 128)

    def band(ref, j, start, count):
        return ref.at[:, pl.ds(start, count), pl.ds(j * 128, 128)]

    def loads(j):
        if j not in inside:
            return [pltpu.make_async_copy(strip(wide_in, j), wide.at[:, j], load_sem.at[j, 0])]
        low = half + tile_rows
        return [
            pltpu.make_async_copy(
                band(tile_in, j - inside[0], 0, tile_rows),
                wide.at[:, j, pl.ds(half, tile_rows), :], load_sem.at[j, 0]),
            pltpu.make_async_copy(
                band(wide_in, j, 0, half), wide.at[:, j, pl.ds(0, half), :], load_sem.at[j, 1]),
            pltpu.make_async_copy(
                band(wide_in, j, low, half), wide.at[:, j, pl.ds(low, half), :], load_sem.at[j, 2]),
        ]

    def save(j):
        return pltpu.make_async_copy(tot.at[:, j], strip(tot_out, j), save_sem.at[j])

    for j in range(blocks):
        for copy in loads(j):
            copy.start()
    slots = counts.shape[0]
    ty, tx = lax.axis_index("ty"), lax.axis_index("tx")
    for n, (u, v) in enumerate(((u_hi, v_hi), (u_lo, v_lo))):
        c, s = tables[2 * n], tables[2 * n + 1]
        u[0:size, 0:size] = c
        u[0:size, size:] = s
        u[size:, 0:size] = -s
        u[size:, size:] = c
        v[0:size, 0:size] = c
        v[0:size, size:] = -s
        v[size:, 0:size] = s
        v[size:, size:] = c
    tot[...] = jnp.zeros_like(tot)
    acc[...] = jnp.zeros_like(acc)
    edge = size // 128
    inner = slice(edge, edge + tile_cols // 128)
    denbuf[inner, size:size + tile_rows, :] = jnp.zeros((tile_cols // 128, tile_rows, 128), jnp.float32)
    pad = jnp.zeros((size, 128), jnp.float32)
    wider = size + 128

    def spread(piece, shift):
        return pltpu.roll(jnp.concatenate([piece, pad], axis=1), shift, axis=1)

    def from_left(m_hi, m_lo, re, im):
        hi, lo = split(jnp.concatenate([re, im], axis=0))
        out = mm(m_hi[...], hi) + (mm(m_hi[...], lo) + mm(m_lo[...], hi))
        return out[:size], out[size:]

    def from_right(m_hi, m_lo, re, im):
        hi, lo = split(jnp.concatenate([re, im], axis=1))
        out = mm(hi, m_hi[...]) + (mm(lo, m_hi[...]) + mm(hi, m_lo[...]))
        return out[:, :size], out[:, size:]

    def one_den(n, carry):
        k, s = n // slots, n % slots
        row = metas[k, 0, s] - ty * tile_rows
        col = metas[k, 0, slots + s] - tx * tile_cols
        there_r, there_c = ty + k // 3 - 1, tx + k % 3 - 1
        there = (there_r >= 0) & (there_r < shape["ty"]) & (there_c >= 0) & (there_c < shape["tx"])
        meets = (row > -size) & (row < tile_rows) & (col > -size) & (col < tile_cols)

        @pl.when(there & meets & (s < metas[k, 0, 2 * slots]))
        def _():
            q = probe[0] * probe[0] + probe[1] * probe[1]
            at = col + size
            value = spread(q, at % 128)
            for i in range(wider // 128):
                where = (at // 128 + i, pl.ds(row + size, size), slice(None))
                denbuf[where] += value[:, i * 128:(i + 1) * 128]
        return carry

    lax.fori_loop(0, 9 * slots, one_den, 0)
    own = denbuf[inner, size:size + tile_rows, :]
    for j in range(tile_cols // 128):
        den[:, j * 128:(j + 1) * 128] = own[j]
    most = jnp.max(own, axis=0)
    den_max[...] = jnp.broadcast_to(jnp.max(jnp.max(most, axis=0, keepdims=True), axis=1, keepdims=True), den_max.shape)
    for j in range(blocks):
        for copy in loads(j):
            copy.wait()

    def one_slot(s, carry):
        row = metas[4, 0, s] - ty * tile_rows + half
        at = metas[4, 0, slots + s] - tx * tile_cols + half
        first = at // 128
        shift = at % 128
        back_shift = (wider - shift) % wider

        def patch(ch):
            found = [wide[ch, first + i, pl.ds(row, size), :] for i in range(wider // 128)]
            return pltpu.roll(jnp.concatenate(found, axis=1), back_shift, axis=1)[:, :size]

        def deposit(ch, piece):
            value = spread(piece, shift)
            for i in range(wider // 128):
                tot[ch, first + i, pl.ds(row, size), :] += value[:, i * 128:(i + 1) * 128]

        x_re, x_im = patch(0), patch(1)
        q_re, q_im = probe[0], probe[1]
        p_re = q_re * x_re - q_im * x_im
        p_im = q_re * x_im + q_im * x_re
        f_re, f_im = from_right(v_hi, v_lo, *from_left(u_hi, u_lo, p_re, p_im))
        amplitude = 0.05 * jnp.sqrt(counts[s].astype(jnp.float32))
        factor = amplitude * lax.rsqrt(jnp.maximum(f_re * f_re + f_im * f_im, 0.0625))
        b_re, b_im = from_right(u_hi, u_lo, *from_left(v_hi, v_lo, f_re * factor, f_im * factor))
        d_re, d_im = b_re - p_re, b_im - p_im
        deposit(0, q_re * d_re + q_im * d_im)
        deposit(1, q_re * d_im - q_im * d_re)
        acc[0] += x_re * d_re + x_im * d_im
        acc[1] += x_re * d_im - x_im * d_re
        acc[2] += x_re * x_re + x_im * x_im
        return carry

    lax.fori_loop(0, metas[4, 0, 2 * slots], one_slot, 0)
    for j in range(blocks):
        save(j).start()
    each = size // shape["ty"]
    for t in range(shape["ty"]):
        for ch in range(3):
            sums[t % 2, t // 2, ch * each:(ch + 1) * each, :] = acc[ch, t * each:(t + 1) * each, :]
    for j in range(blocks):
        save(j).wait()


def fold_kernel(shape, half, tile_in, tot, den_in, den_max, sums, probe_in, out, out_probe,
                tile, den, probe_rows, s0, centre, rim_v, rim_h, rim_c, r1, s1, r2, s2, r3, s3, g4, pk_a, pk_b, pk_c,
                fsend, frecv, send1, recv1, send2, recv2, send3, recv3, send4, recv4,
                ksend, krecv, lsend, lrecv, msend, mrecv, local):
    rows, cols = tile.shape[1], tile.shape[2]
    n_ty, n_tx, n_an = shape["ty"], shape["tx"], shape["angle"]
    ty, tx, an = lax.axis_index("ty"), lax.axis_index("tx"), lax.axis_index("angle")
    core, z = ty % 2, ty // 2
    n_z = n_ty // 2
    group = n_an * n_tx
    gid = an * n_tx + tx
    part = sums.shape[3] // n_an
    diagonals = [d for d in BESIDE if d[0] and d[1]]
    barrier = pltpu.get_barrier_semaphore()

    def signal(where):
        pl.semaphore_signal(barrier, inc=1, device_id=where, device_id_type=MESH)

    def member(d):
        g = (gid + d) % group
        return g, {"angle": g // n_tx, "tx": g % n_tx}

    for d in range(1, n_ty):
        signal({"ty": (ty + d) % n_ty})
    for d in range(1, group):
        signal(member(d)[1])
    for dy, dx in diagonals:
        @pl.when(present(dy, dx, shape))
        def _():
            signal(neighbour(dy, dx))
    each = probe_rows.shape[1]
    own_rows = pl.ds(pl.multiple_of(ty * each, each), each)
    load = pltpu.make_async_copy(
        at2(tot, wide_part(0, rows, half), wide_part(0, cols, half)), centre, local.at[0])
    load_sums = pltpu.make_async_copy(sums.at[core], s0, local.at[1])
    load_tile = pltpu.make_async_copy(tile_in, tile, local.at[2])
    load_den = pltpu.make_async_copy(den_in, den, local.at[3])
    load_probe = pltpu.make_async_copy(probe_in.at[:, own_rows, :], probe_rows, local.at[4])
    for copy in (load_sums, load, load_tile, load_den, load_probe):
        copy.start()
    n_row, n_col = beside_counts(shape)
    pl.semaphore_wait(barrier, n_ty - 1 + group - 1 + n_row * n_col)

    def rdma(src, dst, s_sem, r_sem, where):
        return pltpu.make_async_remote_copy(
            src_ref=src, dst_ref=dst, send_sem=s_sem, recv_sem=r_sem,
            device_id=where, device_id_type=MESH)

    def landing(dy, dx):
        if dx == 0:
            return rim_v.at[(dy + 1) // 2]
        if dy == 0:
            return rim_h.at[(dx + 1) // 2]
        return rim_c.at[(dy + 1) + (dx + 1) // 2]

    early = half * 5 // 8 // 8 * 8

    def fold(dy, dx, piece=0):
        k = slot_of(dy, dx) + 9 * piece
        part_rows, part_cols = wide_part(dy, rows, half), wide_part(dx, cols, half)
        place = landing(dy, dx)
        if dx == 0:
            begin, stop = (0, early) if piece == 0 else (early, half)
            part_rows = slice(part_rows.start + begin, part_rows.start + stop)
            place = place.at[:, pl.ds(begin, stop - begin), :]
        return rdma(at2(tot, part_rows, part_cols), place, fsend.at[k], frecv.at[k], neighbour(dy, dx))

    def start_folds(which):
        for dy, dx, piece in which:
            @pl.when(present(dy, dx, shape))
            def _():
                fold(dy, dx, piece).start()

    pair = {"ty": ty + 1 - 2 * core}
    c1 = rdma(sums.at[1 - core], r1, send1.at[0], recv1.at[0], pair)
    c1.start()
    for d in range(1, group):
        g, where = member(d)
        rdma(den_max, pk_a.at[gid], ksend.at[d], krecv.at[gid], where).start()
    start_folds([(-1, 0, 0), (1, 0, 0), (0, -1, 0), (0, 1, 0)])

    pk_a[pl.ds(gid, 1)] = den_max[...][None]
    c1.wait()
    load_sums.wait()
    s1[...] = s0[...] + r1[...]

    def lanes(ref, a):
        return ref.at[:, :, pl.ds(pl.multiple_of(a * part, part), part)]

    def stage2(d):
        a = (an + d) % n_an
        return rdma(lanes(s1, a), r2.at[an], send2.at[d], recv2.at[an], {"angle": a})

    for d in range(1, n_an):
        stage2(d).start()
    for d in range(1, group):
        g, where = member(d)
        rdma(den_max, pk_a.at[g], ksend.at[d], krecv.at[g], where).wait()
    peak = pk_a[0]
    for g in range(1, group):
        peak = jnp.maximum(peak, pk_a[g])
    pk_b[pl.ds(ty, 1)] = peak[None]
    for d in range(1, n_ty):
        rdma(pk_b.at[ty], pk_b.at[ty], lsend.at[d], lrecv.at[ty], {"ty": (ty + d) % n_ty}).start()
    for d in range(1, n_an):
        a = (an + d) % n_an
        rdma(lanes(s1, a), r2.at[a], send2.at[d], recv2.at[a], {"angle": a}).wait()
    mine = s1[:, :, pl.ds(pl.multiple_of(an * part, part), part)]
    for d in range(1, n_an):
        mine = mine + r2[(an + d) % n_an]
    s2[...] = mine

    for d in range(1, n_z):
        o = (z + d) % n_z
        rdma(s2.at[o], r3.at[z], send3.at[d], recv3.at[z], {"ty": o * 2 + core}).start()
    start_folds([(-1, 0, 1), (1, 0, 1)] + [(dy, dx, 0) for dy, dx in diagonals])
    for d in range(1, n_z):
        o = (z + d) % n_z
        rdma(s2.at[o], r3.at[o], send3.at[d], recv3.at[o], {"ty": o * 2 + core}).wait()
    total = s2[z]
    for d in range(1, n_z):
        total = total + r3[(z + d) % n_z]
    s3[...] = total
    g4[pl.ds(gid, 1)] = total[None]

    for d in range(1, group):
        g, where = member(d)
        rdma(s3, g4.at[gid], send4.at[d], recv4.at[gid], where).start()
    for d in range(1, group):
        g, where = member(d)
        rdma(s3, g4.at[g], send4.at[d], recv4.at[g], where).wait()
    pieces = []
    for a in range(n_an):
        piece = g4[a * n_tx]
        for t in range(1, n_tx):
            piece = piece + g4[a * n_tx + t]
        pieces.append(piece)
    full = jnp.concatenate(pieces, axis=1)
    p_re, p_im, p_den = full[:each], full[each:2 * each], full[2 * each:]

    def top(value):
        return jnp.max(jnp.max(value, axis=0, keepdims=True), axis=1, keepdims=True)

    pk_c[pl.ds(ty, 1)] = jnp.broadcast_to(top(p_den), den_max.shape)[None]
    for d in range(1, n_ty):
        rdma(pk_c.at[ty], pk_c.at[ty], msend.at[d], mrecv.at[ty], {"ty": (ty + d) % n_ty}).start()

    for copy in (load, load_tile, load_den, load_probe):
        copy.wait()
    for dy, dx in [(0, -1), (0, 1), (-1, 0), (1, 0)] + diagonals:
        @pl.when(present(dy, dx, shape))
        def _():
            for piece in (0, 1) if dx == 0 else (0,):
                fold(dy, dx, piece).wait_send()
                fold(-dy, -dx, piece).wait_recv()
            r, c = edge_part(dy, rows, half), edge_part(dx, cols, half)
            centre[:, r, c] += landing(-dy, -dx)[...]
    for d in range(1, n_ty):
        o = (ty + d) % n_ty
        rdma(pk_b.at[ty], pk_b.at[o], lsend.at[d], lrecv.at[o], {"ty": o}).wait()
    peak = pk_b[0]
    for t in range(1, n_ty):
        peak = jnp.maximum(peak, pk_b[t])
    scale = 1.0 / (den[...] + 0.1 * peak[0:1, 0:1])
    centre[0] = tile[0] + centre[0] * scale
    centre[1] = tile[1] + centre[1] * scale
    store = pltpu.make_async_copy(centre, out, local.at[5])
    store.start()

    for d in range(1, n_ty):
        o = (ty + d) % n_ty
        rdma(pk_c.at[ty], pk_c.at[o], msend.at[d], mrecv.at[o], {"ty": o}).wait()
    peak = pk_c[0]
    for t in range(1, n_ty):
        peak = jnp.maximum(peak, pk_c[t])
    scale = 1.0 / (p_den + 0.1 * peak[0:1, 0:1])
    out_probe[0] = probe_rows[0] + p_re * scale
    out_probe[1] = probe_rows[1] + p_im * scale
    store.wait()


def table_values(length):
    ids = np.arange(length)
    phase = 2.0 * math.pi / length * (np.outer(ids, ids) % length)
    cos, sin = np.cos(phase) / math.sqrt(length), np.sin(phase) / math.sqrt(length)
    parts = []
    for value in (cos, sin):
        high = value.astype(jnp.bfloat16)
        low = (value - high.astype(np.float64)).astype(jnp.bfloat16)
        parts.append((high, low))
    return np.stack([parts[0][0], parts[1][0], parts[0][1], parts[1][1]])


def body(shape, object_slices, probe_field, positions, live_slots, photon_counts):
    f32 = jnp.float32
    dma = pltpu.SemaphoreType.DMA
    size = probe_field.shape[1]
    half = size // 2
    tile = object_slices[0]
    _, rows, cols = tile.shape
    spots = positions[0, 0, 0]
    slots = spots.shape[0]
    vmem = pl.BlockSpec(memory_space=pltpu.VMEM)
    smem = pl.BlockSpec(memory_space=pltpu.SMEM)
    anywhere = pl.BlockSpec(memory_space=pl.ANY)
    line = jnp.concatenate([spots[:, 0], spots[:, 1], live_slots[0, 0]])
    meta = jnp.broadcast_to(jnp.pad(line, (0, 128 - line.shape[0]))[None], (8, 128))
    wide, metas = pl.pallas_call(
        functools.partial(halo_kernel, shape, half),
        out_shape=(
            jax.ShapeDtypeStruct((2, rows + size, cols + size), f32),
            jax.ShapeDtypeStruct((9, 8, 128), jnp.int32),
        ),
        in_specs=[anywhere, vmem],
        out_specs=(anywhere, anywhere),
        scratch_shapes=[dma((9,)), dma((9,)), dma((9,)), dma((9,)), dma((2,))],
        cost_estimate=pl.CostEstimate(flops=10**10, bytes_accessed=4 * tile.size, transcendentals=0),
        compiler_params=pltpu.CompilerParams(
            collective_id=0, has_side_effects=True, vmem_limit_bytes=HALO_VMEM),
    )(tile, meta)

    n_ty, n_tx, n_an = shape["ty"], shape["tx"], shape["angle"]
    n_z, each, group = n_ty // 2, size // n_ty, n_an * n_tx
    part = size // n_an
    tot, den, den_max, sums = pl.pallas_call(
        functools.partial(compute_kernel, shape, rows, cols),
        out_shape=(
            jax.ShapeDtypeStruct((2, rows + size, cols + size), f32),
            jax.ShapeDtypeStruct((rows, cols), f32),
            jax.ShapeDtypeStruct((8, 128), f32),
            jax.ShapeDtypeStruct((2, n_z, 3 * each, size), f32),
        ),
        in_specs=[smem, anywhere, anywhere, vmem, vmem, vmem],
        out_specs=(anywhere, vmem, vmem, vmem),
        scratch_shapes=[
            pltpu.VMEM((3, size, size), f32),
            pltpu.VMEM(((cols + 2 * size) // 128, rows + 2 * size, 128), f32),
        ] + [pltpu.VMEM((2 * size, 2 * size), jnp.bfloat16)] * 4 + [
            pltpu.VMEM((2, (cols + size) // 128, rows + size, 128), f32)] * 2 + [
            dma(((cols + size) // 128, 3)), dma(((cols + size) // 128,))],
        compiler_params=pltpu.CompilerParams(vmem_limit_bytes=VMEM_LIMIT),
    )(metas, tile, wide, probe_field, photon_counts[0, 0, 0], jnp.asarray(table_values(size)))

    return pl.pallas_call(
        functools.partial(fold_kernel, shape, half),
        out_shape=(
            jax.ShapeDtypeStruct((2, rows, cols), f32),
            jax.ShapeDtypeStruct((2, each, size), f32),
        ),
        in_specs=[anywhere, anywhere, anywhere, vmem, anywhere, anywhere],
        out_specs=(anywhere, vmem),
        scratch_shapes=[
            pltpu.VMEM((2, rows, cols), f32),
            pltpu.VMEM((rows, cols), f32),
            pltpu.VMEM((2, each, size), f32),
            pltpu.VMEM((n_z, 3 * each, size), f32),
            pltpu.VMEM((2, rows, cols), f32),
            pltpu.VMEM((2, 2, half, cols), f32),
            pltpu.VMEM((2, 2, rows, half), f32),
            pltpu.VMEM((4, 2, half, half), f32),
            pltpu.VMEM((n_z, 3 * each, size), f32),
            pltpu.VMEM((n_z, 3 * each, size), f32),
            pltpu.VMEM((n_an, n_z, 3 * each, part), f32),
            pltpu.VMEM((n_z, 3 * each, part), f32),
            pltpu.VMEM((n_z, 3 * each, part), f32),
            pltpu.VMEM((3 * each, part), f32),
            pltpu.VMEM((group, 3 * each, part), f32),
            pltpu.VMEM((group, 8, 128), f32),
            pltpu.VMEM((n_ty, 8, 128), f32),
            pltpu.VMEM((n_ty, 8, 128), f32),
            dma((18,)), dma((18,)), dma((1,)), dma((1,)), dma((n_an,)), dma((n_an,)),
            dma((n_z,)), dma((n_z,)), dma((group,)), dma((group,)),
            dma((group,)), dma((group,)), dma((n_ty,)), dma((n_ty,)), dma((n_ty,)), dma((n_ty,)),
            dma((6,)),
        ],
        compiler_params=pltpu.CompilerParams(
            collective_id=1, has_side_effects=True, vmem_limit_bytes=FOLD_VMEM),
    )(tile, tot, den, den_max, sums, probe_field)


def solution(mesh):
    shape = dict(mesh.shape)

    def step(*args):
        new_tile, new_probe = body(shape, *args)
        return new_tile[None], new_probe

    return jax.shard_map(
        step,
        mesh=mesh,
        in_specs=(
            P("angle", None, "ty", "tx"),
            P(),
            P("angle", "ty", "tx", None, None),
            P("angle", "ty", "tx"),
            P("angle", "ty", "tx", None, None, None),
        ),
        out_specs=(P("angle", None, "ty", "tx"), P(None, "ty", None)),
        check_vma=False,
    )
```

```python
import functools
import math

import jax
import jax.numpy as jnp
import numpy as np
from jax import lax
from jax.experimental import pallas as pl
from jax.experimental.pallas import tpu as pltpu
from jax.sharding import PartitionSpec as P

MESH = pl.DeviceIdType.MESH
MIB = 1024 * 1024
HALO_VMEM = 4 * MIB
VMEM_LIMIT = 32 * MIB
FOLD_VMEM = 14 * MIB
AROUND = tuple((dy, dx) for dy in (-1, 0, 1) for dx in (-1, 0, 1))
BESIDE = tuple(d for d in AROUND if d != (0, 0))


def slot_of(dy, dx):
    return (dy + 1) * 3 + dx + 1


def present(dy, dx, shape):
    row = lax.axis_index("ty") + dy
    col = lax.axis_index("tx") + dx
    return (row >= 0) & (row < shape["ty"]) & (col >= 0) & (col < shape["tx"])


def beside_counts(shape):
    found = []
    for axis in ("ty", "tx"):
        at = lax.axis_index(axis)
        found.append(jnp.where(at > 0, 1, 0) + jnp.where(at < shape[axis] - 1, 1, 0))
    return found


def neighbour(dy, dx):
    return {"ty": lax.axis_index("ty") + dy, "tx": lax.axis_index("tx") + dx}


def edge_part(step, size, half):
    return {-1: slice(0, half), 0: slice(0, size), 1: slice(size - half, size)}[step]


def wide_part(step, size, half):
    return {
        -1: slice(0, half),
        0: slice(half, half + size),
        1: slice(half + size, size + 2 * half),
    }[step]


def at2(ref, rows, cols):
    return ref.at[:, pl.ds(rows.start, rows.stop - rows.start), pl.ds(cols.start, cols.stop - cols.start)]


def halo_kernel(shape, half, tile, meta, wide, metas, send, recv, msend, mrecv, local):
    rows, cols = tile.shape[1], tile.shape[2]
    barrier = pltpu.get_barrier_semaphore()
    for dy, dx in BESIDE:
        @pl.when(present(dy, dx, shape))
        def _():
            pl.semaphore_signal(barrier, inc=1, device_id=neighbour(dy, dx), device_id_type=MESH)
    own_meta = pltpu.make_async_copy(meta, metas.at[4], local.at[1])
    own_meta.start()
    n_row, n_col = beside_counts(shape)
    pl.semaphore_wait(barrier, n_row + n_col + n_row * n_col)

    def copies(dy, dx, k):
        src = at2(tile, edge_part(dy, rows, half), edge_part(dx, cols, half))
        dst = at2(wide, wide_part(-dy, rows, half), wide_part(-dx, cols, half))
        data = pltpu.make_async_remote_copy(
            src_ref=src, dst_ref=dst, send_sem=send.at[k], recv_sem=recv.at[k],
            device_id=neighbour(dy, dx), device_id_type=MESH)
        note = pltpu.make_async_remote_copy(
            src_ref=meta, dst_ref=metas.at[slot_of(-dy, -dx)], send_sem=msend.at[k],
            recv_sem=mrecv.at[k], device_id=neighbour(dy, dx), device_id_type=MESH)
        return data, note

    order = sorted(BESIDE, key=lambda d: abs(d[1]))
    for dy, dx in order:
        @pl.when(present(dy, dx, shape))
        def _():
            data, note = copies(dy, dx, slot_of(dy, dx))
            data.start()
            note.start()
    for dy, dx in order:
        @pl.when(present(dy, dx, shape))
        def _():
            data, note = copies(dy, dx, slot_of(dy, dx))
            data.wait_send()
            note.wait_send()
            data, note = copies(-dy, -dx, slot_of(-dy, -dx))
            data.wait_recv()
            note.wait_recv()
    own_meta.wait()


def split(value):
    high = value.astype(jnp.bfloat16)
    low = (value - high.astype(jnp.float32)).astype(jnp.bfloat16)
    return high, low


def mm(a, b):
    return lax.dot_general(a, b, (((1,), (0,)), ((), ())), preferred_element_type=jnp.float32)


def compute_kernel(shape, tile_rows, tile_cols, metas, tile_in, wide_in, probe, counts, tables,
                   tot_out, den, den_max, sums, acc, denbuf, u_beside, v_beside, u_below, v_below, wide, tot,
                   load_sem, save_sem):
    size = probe.shape[1]
    half = size // 2
    blocks = wide.shape[1]

    def strip(ref, j):
        return ref.at[:, :, pl.ds(j * 128, 128)]

    inside = range(half // 128, blocks - half // 128)

    def band(ref, j, start, count):
        return ref.at[:, pl.ds(start, count), pl.ds(j * 128, 128)]

    def loads(j):
        if j not in inside:
            return [pltpu.make_async_copy(strip(wide_in, j), wide.at[:, j], load_sem.at[j, 0])]
        low = half + tile_rows
        return [
            pltpu.make_async_copy(
                band(tile_in, j - inside[0], 0, tile_rows),
                wide.at[:, j, pl.ds(half, tile_rows), :], load_sem.at[j, 0]),
            pltpu.make_async_copy(
                band(wide_in, j, 0, half), wide.at[:, j, pl.ds(0, half), :], load_sem.at[j, 1]),
            pltpu.make_async_copy(
                band(wide_in, j, low, half), wide.at[:, j, pl.ds(low, half), :], load_sem.at[j, 2]),
        ]

    def save(j):
        return pltpu.make_async_copy(tot.at[:, j], strip(tot_out, j), save_sem.at[j])

    for j in range(blocks):
        for copy in loads(j):
            copy.start()
    slots = counts.shape[0]
    ty, tx = lax.axis_index("ty"), lax.axis_index("tx")
    for n, level in enumerate((0, 0, 1)):
        c, s = tables[2 * level], tables[2 * level + 1]
        at = 2 * size * n
        for beside, below, top_right, low_left in ((u_beside, u_below, s, -s), (v_beside, v_below, -s, s)):
            quads = ((0, 0, c), (0, size, top_right), (size, 0, low_left), (size, size, c))
            for row, col, value in quads:
                beside[row:row + size, at + col:at + col + size] = value
                below[at + row:at + row + size, col:col + size] = value
    tot[...] = jnp.zeros_like(tot)
    acc[...] = jnp.zeros_like(acc)
    edge = size // 128
    inner = slice(edge, edge + tile_cols // 128)
    denbuf[inner, size:size + tile_rows, :] = jnp.zeros((tile_cols // 128, tile_rows, 128), jnp.float32)
    pad = jnp.zeros((size, 128), jnp.float32)
    wider = size + 128

    def spread(piece, shift):
        return pltpu.roll(jnp.concatenate([piece, pad], axis=1), shift, axis=1)

    def from_left(m, re, im):
        (rh, rl), (ih, il) = split(re), split(im)
        out = mm(m[...], jnp.concatenate([rh, ih, rl, il, rh, ih], axis=0))
        return out[:size], out[size:]

    def from_right(m, re, im):
        (rh, rl), (ih, il) = split(re), split(im)
        out = mm(jnp.concatenate([rh, ih, rl, il, rh, ih], axis=1), m[...])
        return out[:, :size], out[:, size:]

    def one_den(n, carry):
        k, s = n // slots, n % slots
        row = metas[k, 0, s] - ty * tile_rows
        col = metas[k, 0, slots + s] - tx * tile_cols
        there_r, there_c = ty + k // 3 - 1, tx + k % 3 - 1
        there = (there_r >= 0) & (there_r < shape["ty"]) & (there_c >= 0) & (there_c < shape["tx"])
        meets = (row > -size) & (row < tile_rows) & (col > -size) & (col < tile_cols)

        @pl.when(there & meets & (s < metas[k, 0, 2 * slots]))
        def _():
            q = probe[0] * probe[0] + probe[1] * probe[1]
            at = col + size
            value = spread(q, at % 128)
            for i in range(wider // 128):
                where = (at // 128 + i, pl.ds(row + size, size), slice(None))
                denbuf[where] += value[:, i * 128:(i + 1) * 128]
        return carry

    lax.fori_loop(0, 9 * slots, one_den, 0)
    own = denbuf[inner, size:size + tile_rows, :]
    for j in range(tile_cols // 128):
        den[:, j * 128:(j + 1) * 128] = own[j]
    most = jnp.max(own, axis=0)
    den_max[...] = jnp.broadcast_to(jnp.max(jnp.max(most, axis=0, keepdims=True), axis=1, keepdims=True), den_max.shape)
    for j in range(blocks):
        for copy in loads(j):
            copy.wait()

    def one_slot(s, carry):
        row = metas[4, 0, s] - ty * tile_rows + half
        at = metas[4, 0, slots + s] - tx * tile_cols + half
        first = at // 128
        shift = at % 128
        back_shift = (wider - shift) % wider

        def patch(ch):
            found = [wide[ch, first + i, pl.ds(row, size), :] for i in range(wider // 128)]
            return pltpu.roll(jnp.concatenate(found, axis=1), back_shift, axis=1)[:, :size]

        def deposit(ch, piece):
            value = spread(piece, shift)
            for i in range(wider // 128):
                tot[ch, first + i, pl.ds(row, size), :] += value[:, i * 128:(i + 1) * 128]

        x_re, x_im = patch(0), patch(1)
        q_re, q_im = probe[0], probe[1]
        p_re = q_re * x_re - q_im * x_im
        p_im = q_re * x_im + q_im * x_re
        f_re, f_im = from_right(v_below, *from_left(u_beside, p_re, p_im))
        amplitude = 0.05 * jnp.sqrt(counts[s].astype(jnp.float32))
        factor = amplitude * lax.rsqrt(jnp.maximum(f_re * f_re + f_im * f_im, 0.0625))
        b_re, b_im = from_right(u_below, *from_left(v_beside, f_re * factor, f_im * factor))
        d_re, d_im = b_re - p_re, b_im - p_im
        deposit(0, q_re * d_re + q_im * d_im)
        deposit(1, q_re * d_im - q_im * d_re)
        acc[0] += x_re * d_re + x_im * d_im
        acc[1] += x_re * d_im - x_im * d_re
        acc[2] += x_re * x_re + x_im * x_im
        return carry

    lax.fori_loop(0, metas[4, 0, 2 * slots], one_slot, 0)
    for j in range(blocks):
        save(j).start()
    each = size // shape["ty"]
    for t in range(shape["ty"]):
        for ch in range(3):
            sums[t % 2, t // 2, ch * each:(ch + 1) * each, :] = acc[ch, t * each:(t + 1) * each, :]
    for j in range(blocks):
        save(j).wait()


def fold_kernel(shape, half, tile_in, tot, den_in, den_max, sums, probe_in, out, out_probe,
                tile, den, probe_rows, s0, centre, rim_v, rim_h, rim_c, r1, s1, r2, s2, r3, s3, g4, pk_a, pk_b, pk_c,
                fsend, frecv, send1, recv1, send2, recv2, send3, recv3, send4, recv4,
                ksend, krecv, lsend, lrecv, msend, mrecv, local):
    rows, cols = tile.shape[1], tile.shape[2]
    n_ty, n_tx, n_an = shape["ty"], shape["tx"], shape["angle"]
    ty, tx, an = lax.axis_index("ty"), lax.axis_index("tx"), lax.axis_index("angle")
    core, z = ty % 2, ty // 2
    n_z = n_ty // 2
    group = n_an * n_tx
    gid = an * n_tx + tx
    part = sums.shape[3] // n_an
    diagonals = [d for d in BESIDE if d[0] and d[1]]
    barrier = pltpu.get_barrier_semaphore()

    def signal(where):
        pl.semaphore_signal(barrier, inc=1, device_id=where, device_id_type=MESH)

    def member(d):
        g = (gid + d) % group
        return g, {"angle": g // n_tx, "tx": g % n_tx}

    for d in range(1, n_ty):
        signal({"ty": (ty + d) % n_ty})
    for d in range(1, group):
        signal(member(d)[1])
    for dy, dx in diagonals:
        @pl.when(present(dy, dx, shape))
        def _():
            signal(neighbour(dy, dx))
    each = probe_rows.shape[1]
    own_rows = pl.ds(pl.multiple_of(ty * each, each), each)
    load = pltpu.make_async_copy(
        at2(tot, wide_part(0, rows, half), wide_part(0, cols, half)), centre, local.at[0])
    load_sums = pltpu.make_async_copy(sums.at[core], s0, local.at[1])
    load_tile = pltpu.make_async_copy(tile_in, tile, local.at[2])
    load_den = pltpu.make_async_copy(den_in, den, local.at[3])
    load_probe = pltpu.make_async_copy(probe_in.at[:, own_rows, :], probe_rows, local.at[4])
    for copy in (load_sums, load, load_tile, load_den, load_probe):
        copy.start()
    n_row, n_col = beside_counts(shape)
    pl.semaphore_wait(barrier, n_ty - 1 + group - 1 + n_row * n_col)

    def rdma(src, dst, s_sem, r_sem, where):
        return pltpu.make_async_remote_copy(
            src_ref=src, dst_ref=dst, send_sem=s_sem, recv_sem=r_sem,
            device_id=where, device_id_type=MESH)

    def landing(dy, dx):
        if dx == 0:
            return rim_v.at[(dy + 1) // 2]
        if dy == 0:
            return rim_h.at[(dx + 1) // 2]
        return rim_c.at[(dy + 1) + (dx + 1) // 2]

    early = half * 5 // 8 // 8 * 8

    def fold(dy, dx, piece=0):
        k = slot_of(dy, dx) + 9 * piece
        part_rows, part_cols = wide_part(dy, rows, half), wide_part(dx, cols, half)
        place = landing(dy, dx)
        if dx == 0:
            begin, stop = (0, early) if piece == 0 else (early, half)
            part_rows = slice(part_rows.start + begin, part_rows.start + stop)
            place = place.at[:, pl.ds(begin, stop - begin), :]
        return rdma(at2(tot, part_rows, part_cols), place, fsend.at[k], frecv.at[k], neighbour(dy, dx))

    def start_folds(which):
        for dy, dx, piece in which:
            @pl.when(present(dy, dx, shape))
            def _():
                fold(dy, dx, piece).start()

    pair = {"ty": ty + 1 - 2 * core}
    c1 = rdma(sums.at[1 - core], r1, send1.at[0], recv1.at[0], pair)
    c1.start()
    for d in range(1, group):
        g, where = member(d)
        rdma(den_max, pk_a.at[gid], ksend.at[d], krecv.at[gid], where).start()
    start_folds([(-1, 0, 0), (1, 0, 0), (0, -1, 0), (0, 1, 0)])

    pk_a[pl.ds(gid, 1)] = den_max[...][None]
    c1.wait()
    load_sums.wait()
    s1[...] = s0[...] + r1[...]

    def lanes(ref, a):
        return ref.at[:, :, pl.ds(pl.multiple_of(a * part, part), part)]

    def stage2(d):
        a = (an + d) % n_an
        return rdma(lanes(s1, a), r2.at[an], send2.at[d], recv2.at[an], {"angle": a})

    for d in range(1, n_an):
        stage2(d).start()
    for d in range(1, group):
        g, where = member(d)
        rdma(den_max, pk_a.at[g], ksend.at[d], krecv.at[g], where).wait()
    peak = pk_a[0]
    for g in range(1, group):
        peak = jnp.maximum(peak, pk_a[g])
    pk_b[pl.ds(ty, 1)] = peak[None]
    for d in range(1, n_ty):
        rdma(pk_b.at[ty], pk_b.at[ty], lsend.at[d], lrecv.at[ty], {"ty": (ty + d) % n_ty}).start()
    for d in range(1, n_an):
        a = (an + d) % n_an
        rdma(lanes(s1, a), r2.at[a], send2.at[d], recv2.at[a], {"angle": a}).wait()
    mine = s1[:, :, pl.ds(pl.multiple_of(an * part, part), part)]
    for d in range(1, n_an):
        mine = mine + r2[(an + d) % n_an]
    s2[...] = mine

    for d in range(1, n_z):
        o = (z + d) % n_z
        rdma(s2.at[o], r3.at[z], send3.at[d], recv3.at[z], {"ty": o * 2 + core}).start()
    start_folds([(-1, 0, 1), (1, 0, 1)] + [(dy, dx, 0) for dy, dx in diagonals])
    for d in range(1, n_z):
        o = (z + d) % n_z
        rdma(s2.at[o], r3.at[o], send3.at[d], recv3.at[o], {"ty": o * 2 + core}).wait()
    total = s2[z]
    for d in range(1, n_z):
        total = total + r3[(z + d) % n_z]
    s3[...] = total
    g4[pl.ds(gid, 1)] = total[None]

    for d in range(1, group):
        g, where = member(d)
        rdma(s3, g4.at[gid], send4.at[d], recv4.at[gid], where).start()
    for d in range(1, group):
        g, where = member(d)
        rdma(s3, g4.at[g], send4.at[d], recv4.at[g], where).wait()
    pieces = []
    for a in range(n_an):
        piece = g4[a * n_tx]
        for t in range(1, n_tx):
            piece = piece + g4[a * n_tx + t]
        pieces.append(piece)
    full = jnp.concatenate(pieces, axis=1)
    p_re, p_im, p_den = full[:each], full[each:2 * each], full[2 * each:]

    def top(value):
        return jnp.max(jnp.max(value, axis=0, keepdims=True), axis=1, keepdims=True)

    pk_c[pl.ds(ty, 1)] = jnp.broadcast_to(top(p_den), den_max.shape)[None]
    for d in range(1, n_ty):
        rdma(pk_c.at[ty], pk_c.at[ty], msend.at[d], mrecv.at[ty], {"ty": (ty + d) % n_ty}).start()

    for copy in (load, load_tile, load_den, load_probe):
        copy.wait()
    for dy, dx in [(0, -1), (0, 1), (-1, 0), (1, 0)] + diagonals:
        @pl.when(present(dy, dx, shape))
        def _():
            for piece in (0, 1) if dx == 0 else (0,):
                fold(dy, dx, piece).wait_send()
                fold(-dy, -dx, piece).wait_recv()
            r, c = edge_part(dy, rows, half), edge_part(dx, cols, half)
            centre[:, r, c] += landing(-dy, -dx)[...]
    for d in range(1, n_ty):
        o = (ty + d) % n_ty
        rdma(pk_b.at[ty], pk_b.at[o], lsend.at[d], lrecv.at[o], {"ty": o}).wait()
    peak = pk_b[0]
    for t in range(1, n_ty):
        peak = jnp.maximum(peak, pk_b[t])
    scale = 1.0 / (den[...] + 0.1 * peak[0:1, 0:1])
    centre[0] = tile[0] + centre[0] * scale
    centre[1] = tile[1] + centre[1] * scale
    store = pltpu.make_async_copy(centre, out, local.at[5])
    store.start()

    for d in range(1, n_ty):
        o = (ty + d) % n_ty
        rdma(pk_c.at[ty], pk_c.at[o], msend.at[d], mrecv.at[o], {"ty": o}).wait()
    peak = pk_c[0]
    for t in range(1, n_ty):
        peak = jnp.maximum(peak, pk_c[t])
    scale = 1.0 / (p_den + 0.1 * peak[0:1, 0:1])
    out_probe[0] = probe_rows[0] + p_re * scale
    out_probe[1] = probe_rows[1] + p_im * scale
    store.wait()


def table_values(length):
    ids = np.arange(length)
    phase = 2.0 * math.pi / length * (np.outer(ids, ids) % length)
    cos, sin = np.cos(phase) / math.sqrt(length), np.sin(phase) / math.sqrt(length)
    parts = []
    for value in (cos, sin):
        high = value.astype(jnp.bfloat16)
        low = (value - high.astype(np.float64)).astype(jnp.bfloat16)
        parts.append((high, low))
    return np.stack([parts[0][0], parts[1][0], parts[0][1], parts[1][1]])


def body(shape, object_slices, probe_field, positions, live_slots, photon_counts):
    f32 = jnp.float32
    dma = pltpu.SemaphoreType.DMA
    size = probe_field.shape[1]
    half = size // 2
    tile = object_slices[0]
    _, rows, cols = tile.shape
    spots = positions[0, 0, 0]
    slots = spots.shape[0]
    vmem = pl.BlockSpec(memory_space=pltpu.VMEM)
    smem = pl.BlockSpec(memory_space=pltpu.SMEM)
    anywhere = pl.BlockSpec(memory_space=pl.ANY)
    line = jnp.concatenate([spots[:, 0], spots[:, 1], live_slots[0, 0]])
    meta = jnp.broadcast_to(jnp.pad(line, (0, 128 - line.shape[0]))[None], (8, 128))
    wide, metas = pl.pallas_call(
        functools.partial(halo_kernel, shape, half),
        out_shape=(
            jax.ShapeDtypeStruct((2, rows + size, cols + size), f32),
            jax.ShapeDtypeStruct((9, 8, 128), jnp.int32),
        ),
        in_specs=[anywhere, vmem],
        out_specs=(anywhere, anywhere),
        scratch_shapes=[dma((9,)), dma((9,)), dma((9,)), dma((9,)), dma((2,))],
        cost_estimate=pl.CostEstimate(flops=10**10, bytes_accessed=4 * tile.size, transcendentals=0),
        compiler_params=pltpu.CompilerParams(
            collective_id=0, has_side_effects=True, vmem_limit_bytes=HALO_VMEM),
    )(tile, meta)

    n_ty, n_tx, n_an = shape["ty"], shape["tx"], shape["angle"]
    n_z, each, group = n_ty // 2, size // n_ty, n_an * n_tx
    part = size // n_an
    tot, den, den_max, sums = pl.pallas_call(
        functools.partial(compute_kernel, shape, rows, cols),
        out_shape=(
            jax.ShapeDtypeStruct((2, rows + size, cols + size), f32),
            jax.ShapeDtypeStruct((rows, cols), f32),
            jax.ShapeDtypeStruct((8, 128), f32),
            jax.ShapeDtypeStruct((2, n_z, 3 * each, size), f32),
        ),
        in_specs=[smem, anywhere, anywhere, vmem, vmem, vmem],
        out_specs=(anywhere, vmem, vmem, vmem),
        scratch_shapes=[
            pltpu.VMEM((3, size, size), f32),
            pltpu.VMEM(((cols + 2 * size) // 128, rows + 2 * size, 128), f32),
        ] + [pltpu.VMEM((2 * size, 6 * size), jnp.bfloat16)] * 2 + [
            pltpu.VMEM((6 * size, 2 * size), jnp.bfloat16)] * 2 + [
            pltpu.VMEM((2, (cols + size) // 128, rows + size, 128), f32)] * 2 + [
            dma(((cols + size) // 128, 3)), dma(((cols + size) // 128,))],
        compiler_params=pltpu.CompilerParams(vmem_limit_bytes=VMEM_LIMIT),
    )(metas, tile, wide, probe_field, photon_counts[0, 0, 0], jnp.asarray(table_values(size)))

    return pl.pallas_call(
        functools.partial(fold_kernel, shape, half),
        out_shape=(
            jax.ShapeDtypeStruct((2, rows, cols), f32),
            jax.ShapeDtypeStruct((2, each, size), f32),
        ),
        in_specs=[anywhere, anywhere, anywhere, vmem, anywhere, anywhere],
        out_specs=(anywhere, vmem),
        scratch_shapes=[
            pltpu.VMEM((2, rows, cols), f32),
            pltpu.VMEM((rows, cols), f32),
            pltpu.VMEM((2, each, size), f32),
            pltpu.VMEM((n_z, 3 * each, size), f32),
            pltpu.VMEM((2, rows, cols), f32),
            pltpu.VMEM((2, 2, half, cols), f32),
            pltpu.VMEM((2, 2, rows, half), f32),
            pltpu.VMEM((4, 2, half, half), f32),
            pltpu.VMEM((n_z, 3 * each, size), f32),
            pltpu.VMEM((n_z, 3 * each, size), f32),
            pltpu.VMEM((n_an, n_z, 3 * each, part), f32),
            pltpu.VMEM((n_z, 3 * each, part), f32),
            pltpu.VMEM((n_z, 3 * each, part), f32),
            pltpu.VMEM((3 * each, part), f32),
            pltpu.VMEM((group, 3 * each, part), f32),
            pltpu.VMEM((group, 8, 128), f32),
            pltpu.VMEM((n_ty, 8, 128), f32),
            pltpu.VMEM((n_ty, 8, 128), f32),
            dma((18,)), dma((18,)), dma((1,)), dma((1,)), dma((n_an,)), dma((n_an,)),
            dma((n_z,)), dma((n_z,)), dma((group,)), dma((group,)),
            dma((group,)), dma((group,)), dma((n_ty,)), dma((n_ty,)), dma((n_ty,)), dma((n_ty,)),
            dma((6,)),
        ],
        compiler_params=pltpu.CompilerParams(
            collective_id=1, has_side_effects=True, vmem_limit_bytes=FOLD_VMEM),
    )(tile, tot, den, den_max, sums, probe_field)


def solution(mesh):
    shape = dict(mesh.shape)

    def step(*args):
        new_tile, new_probe = body(shape, *args)
        return new_tile[None], new_probe

    return jax.shard_map(
        step,
        mesh=mesh,
        in_specs=(
            P("angle", None, "ty", "tx"),
            P(),
            P("angle", "ty", "tx", None, None),
            P("angle", "ty", "tx"),
            P("angle", "ty", "tx", None, None, None),
        ),
        out_specs=(P("angle", None, "ty", "tx"), P(None, "ty", None)),
        check_vma=False,
    )
```
